8 devices in a mesh: rep: 1 (over z), tp: 2 (over y), sp: 4 (over x, core).
Axes of the slice: x: 2, y: 2, z: 1, core: 2. Of those that a mesh axis runs over, the one named last changes fastest.
Arguments:
- x_in: bfloat16 [2048, 4608], P(('rep', 'sp'))
- positions: int32 [2048], P(('rep', 'sp'))
- norm_gain: float32 [4608], replicated
- w_q: bfloat16 [4608, 4096], P(None, 'tp')
- w_k: bfloat16 [4608, 2048], P(None, 'tp')
- w_v: bfloat16 [4608, 2048], P(None, 'tp')
- w_o: bfloat16 [4096, 4608], P('tp')
- w_gate: bfloat16 [4608, 36864], P(None, 'tp')
- w_up: bfloat16 [4608, 36864], P(None, 'tp')
- w_down: bfloat16 [36864, 4608], P('tp')
Outputs:
- output 1: bfloat16 [2048, 4608], P(('rep', 'sp'))
- output 2: bfloat16 [2048, 16, 128], P('rep', ('tp', 'sp'))
- output 3: bfloat16 [2048, 16, 128], P('rep', ('tp', 'sp'))
All inputs are finite; a program needn't handle non-finite values.
Results may differ from the reference program's by a relative error of at most 0.00250291.
Values are sent between devices in bfloat16 or wider.
A program may use at most 2.25 GiB of HBM per device.

```python
import math
import jax
import jax.numpy as jnp
from jax import lax

MODEL_DIM = 4608
NUM_HEADS = 32
KV_HEADS = 16
HEAD_DIM = 128
FF_DIM = 36864
TOKENS = 2048
GROUP_DEVS = 8
DOC_COUNT = 8

KV_REPEAT = max(GROUP_DEVS // KV_HEADS, 1)
GROUP_SIZE = NUM_HEADS // KV_HEADS
ROW_BLOCK = min(TOKENS, 64)
NUM_BLOCKS = TOKENS // ROW_BLOCK
EPS = 1e-6
ROPE_BASE = 500000.0
SCORE_SCALE = 1.0 / math.sqrt(HEAD_DIM)


def setup_inputs(seed: int = 0, part: int = 0) -> dict:
    part_keys = jax.random.split(jax.random.fold_in(jax.random.key(seed), part), 3)
    shared_keys = jax.random.split(jax.random.key(seed + 1), 8)

    def weight(key_w, fan_in, fan_out):
        return (jax.random.normal(key_w, (fan_in, fan_out), jnp.float32) * fan_in ** -0.5).astype(jnp.bfloat16)

    noise_part = jax.random.normal(part_keys[0], (DOC_COUNT, TOKENS // DOC_COUNT, MODEL_DIM), jnp.float32)
    doc_means = jax.random.normal(part_keys[1], (DOC_COUNT, 1, MODEL_DIM), jnp.float32)
    x_in = (noise_part + doc_means).reshape(TOKENS, MODEL_DIM).astype(jnp.bfloat16)
    start_pos = jax.random.randint(part_keys[2], (), 0, TOKENS)
    positions = (start_pos + jnp.arange(TOKENS)).astype(jnp.int32)
    norm_gain = 1.0 + 0.3 * jax.random.normal(shared_keys[0], (MODEL_DIM,), jnp.float32)
    return {
        "x_in": x_in,
        "positions": positions,
        "norm_gain": norm_gain,
        "w_q": weight(shared_keys[1], MODEL_DIM, NUM_HEADS * HEAD_DIM),
        "w_k": weight(shared_keys[2], MODEL_DIM, KV_HEADS * HEAD_DIM),
        "w_v": weight(shared_keys[3], MODEL_DIM, KV_HEADS * HEAD_DIM),
        "w_o": weight(shared_keys[4], NUM_HEADS * HEAD_DIM, MODEL_DIM),
        "w_gate": weight(shared_keys[5], MODEL_DIM, FF_DIM),
        "w_up": weight(shared_keys[6], MODEL_DIM, FF_DIM),
        "w_down": weight(shared_keys[7], FF_DIM, MODEL_DIM),
    }


def rotate(vectors, cos_tab, sin_tab):
    half_dim = HEAD_DIM // 2
    lower_part = vectors[..., :half_dim]
    upper_part = vectors[..., half_dim:]
    return jnp.concatenate([lower_part * cos_tab - upper_part * sin_tab, upper_part * cos_tab + lower_part * sin_tab], axis=-1).astype(jnp.bfloat16)


def reference(x_in, positions, norm_gain, w_q, w_k, w_v, w_o, w_gate, w_up, w_down):
    x_f32 = x_in.astype(jnp.float32)
    inv_rms = lax.rsqrt(jnp.mean(x_f32 * x_f32, axis=-1, keepdims=True) + EPS)
    normed = (x_f32 * inv_rms * norm_gain).astype(jnp.bfloat16)
    inv_freq = ROPE_BASE ** (-(jnp.arange(HEAD_DIM // 2, dtype=jnp.float32) * (2.0 / HEAD_DIM)))
    angles = positions.astype(jnp.float32)[:, None] * inv_freq[None, :]
    cos_tab = jnp.cos(angles)[:, None, :]
    sin_tab = jnp.sin(angles)[:, None, :]
    q_rot = rotate(jnp.dot(normed, w_q, preferred_element_type=jnp.float32).reshape(TOKENS, NUM_HEADS, HEAD_DIM), cos_tab, sin_tab)
    k_rot = rotate(jnp.dot(normed, w_k, preferred_element_type=jnp.float32).reshape(TOKENS, KV_HEADS, HEAD_DIM), cos_tab, sin_tab)
    v_val = jnp.dot(normed, w_v, preferred_element_type=jnp.float32).astype(jnp.bfloat16).reshape(TOKENS, KV_HEADS, HEAD_DIM)
    q_grouped = q_rot.reshape(TOKENS, KV_HEADS, GROUP_SIZE, HEAD_DIM).astype(jnp.float32)
    k_f32 = k_rot.astype(jnp.float32)
    v_f32 = v_val.astype(jnp.float32)
    key_idx = jnp.arange(TOKENS)

    def attend_block(block_id):
        q_tile = lax.dynamic_slice_in_dim(q_grouped, block_id * ROW_BLOCK, ROW_BLOCK, axis=0)
        scores = jnp.einsum("qcgd,kcd->cgqk", q_tile, k_f32) * SCORE_SCALE
        query_idx = block_id * ROW_BLOCK + jnp.arange(ROW_BLOCK)
        scores = jnp.where(key_idx[None, :] <= query_idx[:, None], scores, -jnp.inf)
        weights = jnp.exp(scores - jnp.max(scores, axis=-1, keepdims=True))
        weight_total = jnp.sum(weights, axis=-1)
        weighted_sum = jnp.einsum("cgqk,kcd->qcgd", weights.astype(jnp.bfloat16).astype(jnp.float32), v_f32)
        return (weighted_sum / jnp.transpose(weight_total, (2, 0, 1))[..., None]).astype(jnp.bfloat16)

    attn_out = lax.map(attend_block, jnp.arange(NUM_BLOCKS)).reshape(TOKENS, NUM_HEADS * HEAD_DIM)
    attn_proj = jnp.dot(attn_out, w_o, preferred_element_type=jnp.float32)
    gate_acc = jnp.dot(normed, w_gate, preferred_element_type=jnp.float32)
    up_acc = jnp.dot(normed, w_up, preferred_element_type=jnp.float32)
    hidden = (jax.nn.silu(gate_acc) * up_acc).astype(jnp.bfloat16)
    mlp_out = jnp.dot(hidden, w_down, preferred_element_type=jnp.float32)
    y_out = (x_f32 + attn_proj + mlp_out).astype(jnp.bfloat16)
    k_cache = jnp.repeat(k_rot, KV_REPEAT, axis=1)
    v_cache = jnp.repeat(v_val, KV_REPEAT, axis=1)
    return y_out, k_cache, v_cache
```

```python
import functools
import math

import jax
import jax.numpy as jnp
from jax import lax
from jax.experimental import pallas as pl
from jax.experimental.pallas import tpu as pltpu
from jax.sharding import PartitionSpec as P

HEAD_DIM = 128
EPS = 1e-6
ROPE_BASE = 500000.0
EXP2_SCALE = HEAD_DIM ** -0.5 * math.log2(math.e)
VMEM_LIMIT = 63 * 2 ** 20
TILE = 512
SHARED_TILES = (11, 12)


def call_params(**kwargs):
    return pltpu.CompilerParams(vmem_limit_bytes=VMEM_LIMIT, **kwargs)


def rope_tables(positions):
    inv_freq = ROPE_BASE ** (-(jnp.arange(HEAD_DIM // 2, dtype=jnp.float32) * (2.0 / HEAD_DIM)))
    angles = positions.astype(jnp.float32)[:, None] * inv_freq[None, :]
    cos_half, sin_half = jnp.cos(angles), jnp.sin(angles)
    return jnp.concatenate([cos_half, cos_half], axis=-1), jnp.concatenate([-sin_half, sin_half], axis=-1)


def project_kernel(x_ref, gain_ref, cos_ref, sin_ref, w_q_ref, w_k_ref, w_v_ref, normed_ref, send_ref):
    @pl.when(pl.program_id(0) == 0)
    def _():
        rows = 64

        def norm_rows(step, carry):
            sl = pl.ds(pl.multiple_of(step * rows, rows), rows)
            x_f32 = x_ref[sl, :].astype(jnp.float32)
            inv_rms = lax.rsqrt(jnp.mean(x_f32 * x_f32, axis=-1, keepdims=True) + EPS)
            normed_ref[sl, :] = (x_f32 * inv_rms * gain_ref[...]).astype(jnp.bfloat16)
            return carry

        lax.fori_loop(0, x_ref.shape[0] // rows, norm_rows, 0)

    base = 0
    for w_ref, rotated in ((w_q_ref, True), (w_k_ref, True), (w_v_ref, False)):
        acc = jnp.dot(normed_ref[...], w_ref[...], preferred_element_type=jnp.float32)
        for lo in range(0, w_ref.shape[1], HEAD_DIM):
            head = acc[:, lo:lo + HEAD_DIM]
            if rotated:
                head = head * cos_ref[...] + pltpu.roll(head, HEAD_DIM // 2, 1) * sin_ref[...]
            send_ref[0, :, base + lo:base + lo + HEAD_DIM] = head.astype(jnp.bfloat16)
        base += w_ref.shape[1]


def project(x_in, norm_gain, cos_tab, sin_tab, w_q, w_k, w_v, sp_size):
    tokens, width = x_in.shape
    dq, dk = w_q.shape[1] // sp_size, w_k.shape[1] // sp_size
    whole = lambda shape: pl.BlockSpec(shape, lambda d: (0, 0))
    cols = lambda n: pl.BlockSpec((width, n), lambda d: (0, d))
    return pl.pallas_call(
        project_kernel,
        grid=(sp_size,),
        in_specs=[whole((tokens, width)), whole((1, width)), whole((tokens, HEAD_DIM)), whole((tokens, HEAD_DIM)), cols(dq), cols(dk), cols(dk)],
        out_specs=[whole((tokens, width)), pl.BlockSpec((1, tokens, dq + 2 * dk), lambda d: (d, 0, 0))],
        out_shape=[jax.ShapeDtypeStruct((tokens, width), jnp.bfloat16), jax.ShapeDtypeStruct((sp_size, tokens, dq + 2 * dk), jnp.bfloat16)],
        compiler_params=call_params(),
        cost_estimate=pl.CostEstimate(flops=2 * tokens * width * (dq + 2 * dk) * sp_size, bytes_accessed=2 * width * (dq + 2 * dk) * sp_size, transcendentals=0),
        name="project",
    )(x_in, norm_gain.reshape(1, width), cos_tab, sin_tab, w_q, w_k, w_v)


def gate_up_kernel(normed_ref, w_gate_ref, w_up_ref, hidden_ref):
    gate_acc = jnp.dot(normed_ref[...], w_gate_ref[...], preferred_element_type=jnp.float32)
    up_acc = jnp.dot(normed_ref[...], w_up_ref[...], preferred_element_type=jnp.float32)
    hidden_ref[...] = (jax.nn.silu(gate_acc) * up_acc).astype(jnp.bfloat16)


def gate_up(normed, w_gate, w_up, first, count, name):
    tokens, width = normed.shape
    w_spec = pl.BlockSpec((width, TILE), lambda i: (0, first + i))
    return pl.pallas_call(
        gate_up_kernel,
        grid=(count,),
        in_specs=[pl.BlockSpec((tokens, width), lambda i: (0, 0)), w_spec, w_spec],
        out_specs=pl.BlockSpec((tokens, TILE), lambda i: (0, i)),
        out_shape=jax.ShapeDtypeStruct((tokens, count * TILE), jnp.bfloat16),
        compiler_params=call_params(),
        cost_estimate=pl.CostEstimate(flops=4 * tokens * width * TILE * count, bytes_accessed=4 * width * TILE * count, transcendentals=tokens * TILE * count),
        name=name,
    )(normed, w_gate, w_up)


def attend_kernel(q_ref, k_ref, v_ref, out_ref, *, key_step):
    rows = q_ref.shape[0]
    group = q_ref.shape[1] // HEAD_DIM
    tile = pl.program_id(1)
    per_step = key_step // rows
    for step in range(k_ref.shape[0] // key_step):
        keys = (step + 1) * key_step

        @pl.when(tile // per_step == step)
        def _():
            row_idx = tile * rows + lax.broadcasted_iota(jnp.int32, (rows, key_step), 0)
            col_idx = step * key_step + lax.broadcasted_iota(jnp.int32, (rows, key_step), 1)
            for h in range(group):
                q_head = q_ref[:, h * HEAD_DIM:(h + 1) * HEAD_DIM]
                scores = []
                for j in range(step + 1):
                    s = lax.dot_general(q_head, k_ref[j * key_step:(j + 1) * key_step, :], (((1,), (1,)), ((), ())), preferred_element_type=jnp.float32)
                    if j == step:
                        s = jnp.where(col_idx <= row_idx, s, -jnp.inf)
                    scores.append(s)
                top = functools.reduce(jnp.maximum, [jnp.max(s, axis=-1, keepdims=True) for s in scores]) * EXP2_SCALE
                weights = [jnp.exp2(s * EXP2_SCALE - top) for s in scores]
                total = functools.reduce(jnp.add, [jnp.sum(w, axis=-1, keepdims=True) for w in weights])
                packed = jnp.concatenate([w.astype(jnp.bfloat16) for w in weights], axis=-1)
                mixed = jnp.dot(packed, v_ref[0:keys, :], preferred_element_type=jnp.float32)
                out_ref[:, h * HEAD_DIM:(h + 1) * HEAD_DIM] = (mixed / total).astype(jnp.bfloat16)


def attend(qkv, heads, caches):
    tokens = qkv.shape[0]
    rows, key_step = 256, 512
    group = heads // caches
    return pl.pallas_call(
        functools.partial(attend_kernel, key_step=key_step),
        grid=(caches, tokens // rows),
        in_specs=[
            pl.BlockSpec((rows, group * HEAD_DIM), lambda c, i: (i, c)),
            pl.BlockSpec((tokens, HEAD_DIM), lambda c, i: (0, heads + c)),
            pl.BlockSpec((tokens, HEAD_DIM), lambda c, i: (0, heads + caches + c)),
        ],
        out_specs=pl.BlockSpec((rows, group * HEAD_DIM), lambda c, i: (i, c)),
        out_shape=jax.ShapeDtypeStruct((tokens, heads * HEAD_DIM), jnp.bfloat16),
        compiler_params=call_params(),
        cost_estimate=pl.CostEstimate(flops=2 * 2 * tokens * tokens * HEAD_DIM * heads, bytes_accessed=4 * tokens * heads * HEAD_DIM, transcendentals=tokens * tokens * heads // 2),
        name="attend",
    )(qkv, qkv, qkv)


def finish_kernel(x_ref, normed_ref, attn_ref, hid_a_ref, hid_b_ref, w_gate_ref, w_up_ref, w_down_ref, w_o_ref, y_ref,
                  slots, wide, rows_u, part_out, part_in, y_buf,
                  slot_sem, load_sem, x_sem, part_send, part_recv, y_local, y_send, y_recv):
    me = lax.axis_index("tp")
    peer = {"tp": 1 - me}
    half = rows_u.shape[0]
    width = normed_ref.shape[1]
    ff = w_down_ref.shape[0]
    depth = slots.shape[1]
    lead = ff - depth
    tiles = y_buf.shape[0]
    split = hid_a_ref.shape[1]
    shared = split + hid_b_ref.shape[1]
    rest = (ff - shared) // TILE
    srcs, head_cols = attn_ref.shape[0], attn_ref.shape[2]

    def copy(src, dst, sem):
        return pltpu.make_async_copy(src, dst, sem)

    def down_copies(n, k, slot):
        cols = pl.ds(pl.multiple_of(n * TILE, TILE), TILE)
        if k == 0:
            return [copy(w_down_ref.at[pl.ds(0, depth), cols], slots.at[slot], slot_sem.at[slot, 0])]
        return [
            copy(w_down_ref.at[pl.ds(depth, lead), cols], slots.at[slot, pl.ds(0, lead)], slot_sem.at[slot, 0]),
            copy(w_o_ref.at[:, cols], slots.at[slot, pl.ds(lead, depth - lead)], slot_sem.at[slot, 1]),
        ]

    def rest_copies(r, slot):
        cols = pl.ds(pl.multiple_of(shared + r * TILE, TILE), TILE)
        return [
            copy(w_gate_ref.at[:, cols], slots.at[slot, pl.ds(0, width)], slot_sem.at[slot, 0]),
            copy(w_up_ref.at[:, cols], slots.at[slot, pl.ds(width, width)], slot_sem.at[slot, 1]),
        ]

    def start(copies):
        for c in copies:
            c.start()

    def wait(copies):
        for c in copies:
            c.wait()

    def row_loads(row):
        loads = [copy(hid_a_ref.at[pl.ds(row, half), :], wide.at[:, pl.ds(0, split)], load_sem.at[0]),
                 copy(hid_b_ref.at[pl.ds(row, half), :], wide.at[:, pl.ds(split, shared - split)], load_sem.at[1])]
        for s in range(srcs):
            loads.append(copy(attn_ref.at[s, pl.ds(row, half), :], wide.at[:, pl.ds(ff + s * head_cols, head_cols)], load_sem.at[2 + s]))
        return loads

    row_peer = pl.multiple_of((1 - me) * half, half)
    row_mine = pl.multiple_of(me * half, half)

    def part_copy(n):
        return pltpu.make_async_remote_copy(part_out.at[n], part_in.at[n], part_send.at[n], part_recv.at[n], device_id=peer, device_id_type=pl.DeviceIdType.MESH)

    def y_window(n):
        return y_ref.at[pl.ds(row_mine, half), pl.ds(pl.multiple_of(n * TILE, TILE), TILE)]

    def y_copy(n):
        return pltpu.make_async_remote_copy(y_buf.at[n], y_window(n), y_send.at[n], y_recv.at[n], device_id=peer, device_id_type=pl.DeviceIdType.MESH)

    def y_keep(n):
        return copy(y_buf.at[n], y_window(n), y_local.at[n])

    def x_load(n):
        return copy(x_ref.at[pl.ds(row_mine, half), pl.ds(n * TILE, TILE)], y_buf.at[n], x_sem.at[n])

    u_load = copy(normed_ref.at[pl.ds(row_peer, half), :], rows_u, load_sem.at[2 + srcs])
    u_load.start()
    start(rest_copies(0, 0))
    start(rest_copies(1, 1))
    loads = row_loads(row_peer)
    start(loads)
    for n in range(tiles):
        x_load(n).start()

    barrier = pltpu.get_barrier_semaphore()
    pl.semaphore_signal(barrier, inc=1, device_id=peer, device_id_type=pl.DeviceIdType.MESH)
    pl.semaphore_wait(barrier, 1)
    u_load.wait()

    def rest_phase(first):
        def rest_step(r, carry):
            slot = lax.rem(first + r, 3)
            ahead = lax.rem(first + r + 2, 3)
            wait(rest_copies(r, slot))

            @pl.when(r + 2 < rest)
            def _():
                start(rest_copies(r + 2, ahead))

            @pl.when(r + 2 == rest)
            def _():
                start(down_copies(0, 0, ahead))

            @pl.when(r + 2 == rest + 1)
            def _():
                start(down_copies(0, 1, ahead))

            gate_acc = jnp.dot(rows_u[...], slots[slot, 0:width, :], preferred_element_type=jnp.float32)
            up_acc = jnp.dot(rows_u[...], slots[slot, width:2 * width, :], preferred_element_type=jnp.float32)
            cols = pl.ds(pl.multiple_of(shared + r * TILE, TILE), TILE)
            wide[:, cols] = (jax.nn.silu(gate_acc) * up_acc).astype(jnp.bfloat16)
            return carry

        lax.fori_loop(0, rest, rest_step, 0)

    def down_phase(first, begin_tile, finish_tile, after):
        def tile_step(n, carry):
            begin_tile(n)
            for k in range(2):
                slot = lax.rem(first + 2 * n + k, 3)
                ahead = lax.rem(first + 2 * n + k + 2, 3)
                wait(down_copies(n, k, slot))

                @pl.when(n + 1 < tiles)
                def _():
                    start(down_copies(n + 1, k, ahead))

                if after is not None:
                    @pl.when(n + 1 == tiles)
                    def _():
                        start(after(k, ahead))

                if k == 0:
                    part_out[n] = jnp.dot(wide[:, 0:depth], slots[slot], preferred_element_type=jnp.float32)
                else:
                    finish_tile(n, jnp.dot(wide[:, depth:2 * depth], slots[slot], preferred_element_type=jnp.float32))
            return carry

        lax.fori_loop(0, tiles, tile_step, 0)

    rest_phase(0)
    wait(loads)

    def begin_peer(n):
        @pl.when(n > 0)
        def _():
            part_copy(n - 1).start()

    def finish_peer(n, dot):
        part_out[n] = part_out[n] + dot

    down_phase(rest, begin_peer, finish_peer, rest_copies)
    part_copy(tiles - 1).start()

    loads = row_loads(row_mine)
    start(loads)
    u_load = copy(normed_ref.at[pl.ds(row_mine, half), :], rows_u, load_sem.at[2 + srcs])
    u_load.start()
    for n in range(tiles):
        x_load(n).wait()
    u_load.wait()
    rest_phase(rest + 2 * tiles)
    wait(loads)

    def begin_mine(n):
        @pl.when(n > 0)
        def _():
            y_keep(n - 1).start()
            y_copy(n - 1).start()
        part_copy(n).wait_send()

    def finish_mine(n, dot):
        part_copy(n).wait_recv()
        total = y_buf[n].astype(jnp.float32) + (part_out[n] + dot + part_in[n])
        y_buf[n] = total.astype(jnp.bfloat16)

    down_phase(2 * rest + 2 * tiles, begin_mine, finish_mine, None)
    y_keep(tiles - 1).start()
    y_copy(tiles - 1).start()

    def drain(n, carry):
        y_keep(n).wait()
        y_copy(n).wait()
        return carry

    lax.fori_loop(0, tiles, drain, 0)


def finish(x_in, normed, attn, hid_a, hid_b, w_gate, w_up, w_down, w_o):
    tokens, width = x_in.shape
    half = tokens // 2
    ff = w_down.shape[0]
    deep = ff + w_o.shape[0]
    tiles = width // TILE
    anywhere = pl.BlockSpec(memory_space=pl.ANY)
    dma = pltpu.SemaphoreType.DMA
    return pl.pallas_call(
        finish_kernel,
        in_specs=[anywhere] * 9,
        out_specs=anywhere,
        out_shape=jax.ShapeDtypeStruct((tokens, width), jnp.bfloat16),
        scratch_shapes=[
            pltpu.VMEM((3, deep // 2, TILE), jnp.bfloat16),
            pltpu.VMEM((half, deep), jnp.bfloat16),
            pltpu.VMEM((half, width), jnp.bfloat16),
            pltpu.VMEM((tiles, half, TILE), jnp.float32),
            pltpu.VMEM((tiles, half, TILE), jnp.float32),
            pltpu.VMEM((tiles, half, TILE), jnp.bfloat16),
            dma((3, 2)),
            dma((3 + attn.shape[0],)),
            dma((tiles,)), dma((tiles,)), dma((tiles,)), dma((tiles,)), dma((tiles,)), dma((tiles,)),
        ],
        compiler_params=call_params(collective_id=0, has_side_effects=True),
        cost_estimate=pl.CostEstimate(flops=4 * tokens * width * ff, bytes_accessed=4 * width * ff, transcendentals=0),
        name="finish",
    )(x_in, normed, attn, hid_a, hid_b, w_gate, w_up, w_down, w_o)


def solution(mesh):
    sp_size = mesh.shape["sp"]
    row_spec = P(("rep", "sp"), None)
    cache_spec = P("rep", ("tp", "sp"), None)

    def layer_block(x_in, positions, norm_gain, w_q, w_k, w_v, w_o, w_gate, w_up, w_down):
        tok_local = x_in.shape[0]
        heads_dev = w_q.shape[1] // HEAD_DIM // sp_size
        cache_dev = w_k.shape[1] // HEAD_DIM // sp_size
        cos_tab, sin_tab = rope_tables(positions)
        normed, send_buf = project(x_in, norm_gain, cos_tab, sin_tab, w_q, w_k, w_v, sp_size)
        recv_buf = lax.all_to_all(send_buf, "sp", 0, 0, tiled=True)
        hid_a = gate_up(normed, w_gate, w_up, 0, SHARED_TILES[0], "gate_up_a")
        recv_buf, hid_a, normed_b = lax.optimization_barrier((recv_buf, hid_a, normed))
        qkv = recv_buf.reshape(tok_local * sp_size, -1)
        attn_heads = attend(qkv, heads_dev, cache_dev)
        attn_send = attn_heads.reshape(sp_size, tok_local, heads_dev * HEAD_DIM)
        attn_send, normed_c = lax.optimization_barrier((attn_send, normed_b))
        attn_recv = lax.all_to_all(attn_send, "sp", 0, 0, tiled=True)
        hid_b = gate_up(normed_c, w_gate, w_up, SHARED_TILES[0], SHARED_TILES[1], "gate_up_b")
        y_out = finish(x_in, normed_c, attn_recv, hid_a, hid_b, w_gate, w_up, w_down, w_o)
        k_all = qkv[:, heads_dev * HEAD_DIM:(heads_dev + cache_dev) * HEAD_DIM].reshape(-1, cache_dev, HEAD_DIM)
        v_all = qkv[:, (heads_dev + cache_dev) * HEAD_DIM:].reshape(-1, cache_dev, HEAD_DIM)
        return y_out, k_all, v_all

    return jax.shard_map(
        layer_block,
        mesh=mesh,
        in_specs=(row_spec, P(("rep", "sp")), P(None), P(None, "tp"), P(None, "tp"), P(None, "tp"), P("tp", None), P(None, "tp"), P(None, "tp"), P("tp", None)),
        out_specs=(row_spec, cache_spec, cache_spec),
        check_vma=False,
    )
```
